32 devices in a mesh: band: 8 (over z, core), lane: 4 (over y, x).
Axes of the slice: x: 2, y: 2, z: 4, core: 2. Of those that a mesh axis runs over, the one named last changes fastest.
Arguments:
- first_factor: bfloat16 [8192, 4096], P('band', 'lane'), may hold values from -6 to 6
- second_factor: bfloat16 [4096, 2048], P('band', 'lane'), may hold values from -0.09375 to 0.09375
- result_in: float32 [8192, 2048], P('band', 'lane'), may hold values from -6 to 6
- pivot_scale: float32 [4096], replicated, may hold values from 0.25 to 1.75
Outputs:
- updated: float32 [8192, 2048], P('band', 'lane')
The draws below stay inside these ranges and needn't reach their ends.
All inputs are finite; a program needn't handle non-finite values.
Results may differ from the reference program's by a relative error of at most 0.002.
Values may be sent and summed in bfloat16 or wider, within the bound.
A program may use at most 128 MiB of HBM per device.

```python
import jax
import jax.numpy as jnp
from jax import lax

ROWS = 8192
COLS = 2048
INNER = 4096


def level_of(own_key, shape, split, least, top_value):
    factor_of = 1.0
    for axis_at, parts in split:
        steps = jax.random.uniform(jax.random.fold_in(jax.random.fold_in(own_key, 6), axis_at), (parts,), jnp.float32, least / len(split), top_value / len(split))
        factor_of = factor_of * jnp.repeat(jnp.exp(steps), shape[axis_at] // parts).reshape((-1,) + (1,) * (len(shape) - 1 - axis_at))
    return factor_of


def centred(own_key, shape, deviation, bound, split=(), held_as=jnp.bfloat16):
    result = jax.random.normal(own_key, shape, jnp.float32) * deviation
    if len(split) > 0:
        result = level_of(own_key, shape, split, -0.22, 0.18) * result
    return jnp.clip(result, min=-bound, max=bound).astype(held_as)


def setup_inputs(seed: int = 0) -> dict:
    key_list = jax.random.split(jax.random.key(seed), 5)
    first_factor = centred(key_list[0], (ROWS, INNER), 1.0, 6.0, ((0, 8), (1, 4)))
    second_factor = centred(key_list[1], (INNER, COLS), INNER ** -0.5, 0.09375, ((0, 8), (1, 4)))
    result_in = centred(key_list[2], (ROWS, COLS), 1.0, 6.0, ((0, 8), (1, 4)), jnp.float32)
    pivot_scale = jnp.clip(1.0 + 0.15 * jax.random.normal(key_list[3], (INNER,), jnp.float32), 0.25, 1.75)
    return {"first_factor": first_factor, "second_factor": second_factor, "result_in": result_in, "pivot_scale": pivot_scale}


def reference(first_factor, second_factor, result_in, pivot_scale):
    scaled_left = (first_factor.astype(jnp.float32) * pivot_scale).astype(jnp.bfloat16)
    updated = result_in - jnp.dot(scaled_left, second_factor, preferred_element_type=jnp.float32)
    row_power = lax.optimization_barrier(jnp.sum(updated * updated, axis=1))
    updated = updated * lax.rsqrt(row_power / COLS + 1e-06)[:, None]
    return updated
```

```python
import functools

import jax
import jax.numpy as jnp
from jax import lax
from jax.experimental import pallas as pl
from jax.experimental.pallas import tpu as pltpu
from jax.sharding import PartitionSpec as P

MESH = pl.DeviceIdType.MESH
PIECES = 2
TILES = 4


def gathered(first_factor, second_factor, result_in, pivot_scale):
    share = first_factor.shape[1]
    part_scale = lax.dynamic_slice_in_dim(pivot_scale, lax.axis_index("lane") * share, share)
    scaled_left = (first_factor.astype(jnp.float32) * part_scale).astype(jnp.bfloat16)
    left_line = lax.all_gather(scaled_left, "lane", axis=1, tiled=True)
    right = lax.all_gather(second_factor, "band", axis=0, tiled=True)
    updated = result_in - jnp.dot(left_line, right, preferred_element_type=jnp.float32)
    row_power = lax.psum(jnp.sum(updated * updated, axis=1), "lane")
    return (
        updated * lax.rsqrt(row_power / (updated.shape[1] * lax.axis_size("lane")) + 1e-06)[:, None]
    )


def kernel(
    chips, left_hbm, right_hbm, result_hbm, scale_ref, out_ref, power_ref,
    left_raw, left, right, result, outgoing, incoming, kept, norm_out, norm_in,
    load_sem, source_sem, right_sem, up_sem, down_sem, peer_send, peer_recv, part_send, part_recv,
    norm_send, norm_recv,
):
    band, lane = lax.axis_index("band"), lax.axis_index("lane")
    z, core = band // 2, band % 2
    y, x = lane // 2, lane % 2
    peer = (2 * z + 1 - core, lane)
    lane_x, lane_y, lane_d = 2 * y + 1 - x, 2 * (1 - y) + x, 2 * (1 - y) + 1 - x
    above, below = (band + 2, lane), (band - 2, lane)
    depth, width = right_hbm.shape
    half = width // 2
    piece = depth // PIECES
    rows, share = left.shape
    tile = rows // TILES

    load_left = pltpu.make_async_copy(left_hbm, left_raw, load_sem.at[0])
    load_left.start()
    load_result = pltpu.make_async_copy(result_hbm, result, load_sem.at[1])
    load_result.start()

    barrier = pltpu.get_barrier_semaphore()
    for other in (lane_x, lane_y, lane_d):
        pl.semaphore_signal(barrier, inc=1, device_id=(band, other), device_id_type=MESH)
    pl.semaphore_signal(barrier, inc=1, device_id=peer, device_id_type=MESH)

    @pl.when(z < chips - 1)
    def _():
        pl.semaphore_signal(barrier, inc=1, device_id=above, device_id_type=MESH)

    @pl.when(z > 0)
    def _():
        pl.semaphore_signal(barrier, inc=1, device_id=below, device_id_type=MESH)

    pl.semaphore_wait(barrier, 4 + (z + chips - 1) // chips + (2 * chips - 2 - z) // chips)

    def place(slot, part, of_core):
        start = pl.multiple_of(of_core * depth + part * piece, piece)
        return right.at[slot, pl.ds(start, piece), :]

    dx, dy = (x + z % 2) % 2, (y + z // 2) % 2
    slot_0 = 4 * dx * (1 - dy) + 3 * (1 - dx) * dy + 6 * (1 - dx) * (1 - dy)
    slot_1 = dx * dy + 2 * dx * (1 - dy) + 5 * (1 - dx) * dy + 7 * (1 - dx) * (1 - dy)

    def own_block(i, part):
        side = (i + dx * (1 - dy)) % 2
        slot = slot_0 * (1 - side) + slot_1 * side
        block = right_hbm.at[
            pl.ds(part * piece, piece), pl.ds(pl.multiple_of(side * half, half), half)
        ]
        return block, slot

    def send_own(i, part):
        block, slot = own_block(i, part)
        return pltpu.make_async_remote_copy(
            block, place(slot, part, core), source_sem.at[i * PIECES + part],
            right_sem.at[slot * PIECES + part], device_id=(band, z), device_id_type=MESH,
        )

    @pl.when(lane != z)
    def _():
        for i in range(2):
            for part in range(PIECES):
                send_own(i, part).start()

    @pl.when(lane == z)
    def _():
        for i in range(2):
            for part in range(PIECES):
                block, slot = own_block(i, part)
                pltpu.make_async_copy(
                    block, place(slot, part, core), right_sem.at[slot * PIECES + part]
                ).start()

    def along(slot, part, device, send, recv):
        at = slot * PIECES + part
        ref = place(slot, part, core)
        return pltpu.make_async_remote_copy(
            ref, ref, send.at[at], recv.at[at], device_id=device, device_id_type=MESH
        )

    def forward(slot):
        for part in range(PIECES):
            along(slot, part, peer, peer_send, right_sem).wait_recv()

            @pl.when((z >= lane) & (z < chips - 1))
            def _():
                along(slot, part, above, up_sem, right_sem).start()

            @pl.when((z <= lane) & (z > 0))
            def _():
                along(slot, part, below, down_sem, right_sem).start()

            along(slot, part, peer, peer_send, peer_recv).start()

    def await_peer(slot):
        for part in range(PIECES):
            at = slot * PIECES + part
            ref = place(slot, part, 1 - core)
            pltpu.make_async_remote_copy(
                ref, ref, peer_send.at[at], peer_recv.at[at], device_id=peer, device_id_type=MESH
            ).wait_recv()

    def part_copy(buffer, at, other):
        index = buffer * TILES + at
        span = pl.ds(pl.multiple_of(at * tile, tile), tile)
        return pltpu.make_async_remote_copy(
            outgoing.at[buffer, span, :], incoming.at[buffer, span, :], part_send.at[index],
            part_recv.at[index], device_id=(band, other), device_id_type=MESH,
        )

    def product(slot, span):
        return jnp.dot(left[span, :], right[slot], preferred_element_type=jnp.float32)

    def each_tile(body):
        @pl.loop(0, TILES)
        def _(at):
            body(at, pl.ds(pl.multiple_of(at * tile, tile), tile))

    def multiply_send(slot, buffer, other):
        def body(at, span):
            outgoing[buffer, span, :] = product(slot, span).astype(jnp.bfloat16)
            part_copy(buffer, at, other).start()

        each_tile(body)

    def multiply_keep(slot, which):
        def body(at, span):
            kept[which, span, :] = product(slot, span)

        each_tile(body)

    def combine_send(which, arrived, buffer, other):
        def body(at, span):
            part_copy(arrived, at, other).wait_recv()
            total = kept[which, span, :] + incoming[arrived, span, :].astype(jnp.float32)
            outgoing[buffer, span, :] = total.astype(jnp.bfloat16)
            part_copy(buffer, at, other).start()

        each_tile(body)

    def multiply_own(slot, side):
        def body(at, span):
            columns = slice(side * half, (side + 1) * half)
            out_ref[span, columns] = result[span, columns] - product(slot, span)

        each_tile(body)

    load_left.wait()
    part_scale = scale_ref[:, pl.ds(pl.multiple_of(lane * share, share), share)]

    def scale_tile(at, span):
        left[span, :] = (left_raw[span, :].astype(jnp.float32) * part_scale).astype(jnp.bfloat16)

    each_tile(scale_tile)

    forward(0)
    await_peer(0)
    multiply_send(0, 0, lane_x)
    forward(1)
    await_peer(1)
    multiply_send(1, 1, lane_y)
    forward(2)
    await_peer(2)
    multiply_keep(2, 0)
    forward(3)
    await_peer(3)
    multiply_keep(3, 1)
    forward(4)
    await_peer(4)
    multiply_send(4, 2, lane_x)
    forward(5)
    await_peer(5)
    multiply_send(5, 3, lane_y)
    forward(6)
    combine_send(0, 1, 4, lane_x)
    combine_send(1, 0, 5, lane_y)
    forward(7)
    load_result.wait()
    await_peer(6)
    multiply_own(6, 0)
    await_peer(7)
    multiply_own(7, 1)

    def finish(at, span):
        for buffer in (2, 3, 4, 5):
            part_copy(buffer, at, lane_x).wait_recv()
        first = out_ref[span, :half] - (
            incoming[2, span, :].astype(jnp.float32) + incoming[5, span, :].astype(jnp.float32)
        )
        second = out_ref[span, half:] - (
            incoming[3, span, :].astype(jnp.float32) + incoming[4, span, :].astype(jnp.float32)
        )
        out_ref[span, :half] = first
        out_ref[span, half:] = second
        power = first * first + second * second
        power = sum(power[:, k : k + 128] for k in range(0, half, 128))
        norm_out[:, span] = jnp.sum(power.T.reshape(16, 8, tile), axis=0)

    each_tile(finish)

    norms = [
        pltpu.make_async_remote_copy(
            norm_out, norm_in.at[k], norm_send.at[k], norm_recv.at[k],
            device_id=(band, other), device_id_type=MESH,
        )
        for k, other in enumerate((lane_x, lane_y, lane_d))
    ]
    for copy in norms:
        copy.start()

    @pl.when(lane != z)
    def _():
        for i in range(2):
            for part in range(PIECES):
                send_own(i, part).wait_send()

    for slot in range(8):
        for part in range(PIECES):
            along(slot, part, peer, peer_send, peer_recv).wait_send()

    @pl.when((z >= lane) & (z < chips - 1))
    def _():
        for slot in range(8):
            for part in range(PIECES):
                along(slot, part, above, up_sem, right_sem).wait_send()

    @pl.when((z <= lane) & (z > 0))
    def _():
        for slot in range(8):
            for part in range(PIECES):
                along(slot, part, below, down_sem, right_sem).wait_send()

    for buffer in range(6):
        for at in range(TILES):
            part_copy(buffer, at, lane_x).wait_send()

    for copy in norms:
        copy.wait()
    power = norm_out[...] + norm_in[0] + norm_in[1] + norm_in[2]
    power = jnp.sum(power, axis=0, keepdims=True)
    power_ref[...] = jnp.broadcast_to(power, (128, rows)).T


def on_device(chips, first_factor, second_factor, result_in, pivot_scale):
    rows, share = first_factor.shape
    depth, width = second_factor.shape
    half = width // 2
    slots = 8 * PIECES
    dma = pltpu.SemaphoreType.DMA
    flops = 2 * rows * share * 4 * width
    updated, power = pl.pallas_call(
        functools.partial(kernel, chips),
        out_shape=(
            jax.ShapeDtypeStruct((rows, width), jnp.float32),
            jax.ShapeDtypeStruct((rows, 128), jnp.float32),
        ),
        in_specs=[pl.BlockSpec(memory_space=pl.ANY)] * 3
        + [pl.BlockSpec(memory_space=pltpu.VMEM)],
        out_specs=[pl.BlockSpec(memory_space=pltpu.VMEM)] * 2,
        scratch_shapes=[
            pltpu.VMEM((rows, share), jnp.bfloat16),
            pltpu.VMEM((rows, share), jnp.bfloat16),
            pltpu.VMEM((8, share, half), jnp.bfloat16),
            pltpu.VMEM((rows, width), jnp.float32),
            pltpu.VMEM((6, rows, half), jnp.bfloat16),
            pltpu.VMEM((6, rows, half), jnp.bfloat16),
            pltpu.VMEM((2, rows, half), jnp.float32),
            pltpu.VMEM((8, rows), jnp.float32),
            pltpu.VMEM((3, 8, rows), jnp.float32),
            dma((2,)),
            dma((2 * PIECES,)),
            dma((slots,)),
            dma((slots,)),
            dma((slots,)),
            dma((slots,)),
            dma((slots,)),
            dma((6 * TILES,)),
            dma((6 * TILES,)),
            dma((3,)),
            dma((3,)),
        ],
        compiler_params=pltpu.CompilerParams(
            collective_id=0, has_side_effects=True, vmem_limit_bytes=48 * 1024 * 1024
        ),
        cost_estimate=pl.CostEstimate(
            flops=flops, bytes_accessed=8 * rows * share, transcendentals=0
        ),
    )(first_factor, second_factor, result_in, pivot_scale.reshape(1, -1))
    return updated * lax.rsqrt(power[:, :1] / (width * lax.axis_size("lane")) + 1e-06)


def solution(mesh):
    bands, lanes = mesh.shape["band"], mesh.shape["lane"]

    def body(first_factor, second_factor, result_in, pivot_scale):
        fits = lanes == 4 and bands == 2 * lanes
        plan = functools.partial(on_device, bands // 2) if fits else gathered
        return plan(first_factor, second_factor, result_in, pivot_scale)

    return jax.shard_map(
        body,
        mesh=mesh,
        in_specs=(P("band", "lane"), P("band", "lane"), P("band", "lane"), P()),
        out_specs=P("band", "lane"),
        check_vma=False,
    )
```

```python
import functools

import jax
import jax.numpy as jnp
from jax import lax
from jax.experimental import pallas as pl
from jax.experimental.pallas import tpu as pltpu
from jax.sharding import PartitionSpec as P

MESH = pl.DeviceIdType.MESH
PIECES = 4
TILES = 4
SWAP = 0
EARLY = 1
VMEM = 48 * 1024 * 1024


def gathered(first_factor, second_factor, result_in, pivot_scale):
    share = first_factor.shape[1]
    part_scale = lax.dynamic_slice_in_dim(pivot_scale, lax.axis_index("lane") * share, share)
    scaled_left = (first_factor.astype(jnp.float32) * part_scale).astype(jnp.bfloat16)
    left_line = lax.all_gather(scaled_left, "lane", axis=1, tiled=True)
    right = lax.all_gather(second_factor, "band", axis=0, tiled=True)
    updated = result_in - jnp.dot(left_line, right, preferred_element_type=jnp.float32)
    row_power = lax.psum(jnp.sum(updated * updated, axis=1), "lane")
    return (
        updated * lax.rsqrt(row_power / (updated.shape[1] * lax.axis_size("lane")) + 1e-06)[:, None]
    )


def kernel(
    chips, left_hbm, right_hbm, result_hbm, scale_ref, out_ref, power_ref,
    left_raw, left, right, result, outgoing, incoming, kept, norm_out, norm_in,
    load_sem, source_sem, right_sem, up_sem, down_sem, peer_send, peer_recv, part_send, part_recv,
    norm_send, norm_recv,
):
    band, lane = lax.axis_index("band"), lax.axis_index("lane")
    z, core = band // 2, band % 2
    y, x = lane // 2, lane % 2
    peer = (2 * z + 1 - core, lane)
    lane_x, lane_y, lane_d = 2 * y + 1 - x, 2 * (1 - y) + x, 2 * (1 - y) + 1 - x
    if SWAP:
        lane_x, lane_y = lane_y, lane_x
    above, below = (band + 2, lane), (band - 2, lane)
    depth, width = right_hbm.shape
    half = width // 2
    piece = depth // PIECES
    rows, share = left.shape
    tile = rows // TILES

    load_left = pltpu.make_async_copy(left_hbm, left_raw, load_sem.at[0])
    load_left.start()
    load_result = pltpu.make_async_copy(result_hbm, result, load_sem.at[1])
    load_result.start()

    barrier = pltpu.get_barrier_semaphore()
    for other in (lane_x, lane_y, lane_d):
        pl.semaphore_signal(barrier, inc=1, device_id=(band, other), device_id_type=MESH)
    pl.semaphore_signal(barrier, inc=1, device_id=peer, device_id_type=MESH)

    @pl.when(z < chips - 1)
    def _():
        pl.semaphore_signal(barrier, inc=1, device_id=above, device_id_type=MESH)

    @pl.when(z > 0)
    def _():
        pl.semaphore_signal(barrier, inc=1, device_id=below, device_id_type=MESH)

    pl.semaphore_wait(barrier, 4 + (z + chips - 1) // chips + (2 * chips - 2 - z) // chips)

    def place(slot, part, of_core):
        start = pl.multiple_of(of_core * depth + part * piece, piece)
        return right.at[slot, pl.ds(start, piece), :]

    dx, dy = (x + z % 2) % 2, (y + z // 2) % 2
    if SWAP:
        dx, dy = dy, dx
    slot_0 = dx * (1 - dy) + 6 * (1 - dx) * dy + 4 * dx * dy
    slot_1 = 7 * (1 - dx) * (1 - dy) + 5 * dx * (1 - dy) + 3 * (1 - dx) * dy + 2 * dx * dy

    def own_block(i, part):
        side = (i + dy) % 2
        slot = slot_0 * (1 - side) + slot_1 * side
        block = right_hbm.at[
            pl.ds(part * piece, piece), pl.ds(pl.multiple_of(side * half, half), half)
        ]
        return block, slot

    def send_own(i, part):
        block, slot = own_block(i, part)
        return pltpu.make_async_remote_copy(
            block, place(slot, part, core), source_sem.at[i * PIECES + part],
            right_sem.at[slot * PIECES + part], device_id=(band, z), device_id_type=MESH,
        )

    @pl.when(lane != z)
    def _():
        for i in range(2):
            for part in range(PIECES):
                send_own(i, part).start()

    @pl.when(lane == z)
    def _():
        for i in range(2):
            for part in range(PIECES):
                block, slot = own_block(i, part)
                pltpu.make_async_copy(
                    block, place(slot, part, core), right_sem.at[slot * PIECES + part]
                ).start()

    def along(slot, part, device, send, recv):
        at = slot * PIECES + part
        ref = place(slot, part, core)
        return pltpu.make_async_remote_copy(
            ref, ref, send.at[at], recv.at[at], device_id=device, device_id_type=MESH
        )

    def forward(slot):
        for part in range(PIECES):
            along(slot, part, peer, peer_send, right_sem).wait_recv()

            @pl.when((z >= lane) & (z < chips - 1))
            def _():
                along(slot, part, above, up_sem, right_sem).start()

            @pl.when((z <= lane) & (z > 0))
            def _():
                along(slot, part, below, down_sem, right_sem).start()

            along(slot, part, peer, peer_send, peer_recv).start()

    def await_peer(slot):
        for part in range(PIECES):
            at = slot * PIECES + part
            ref = place(slot, part, 1 - core)
            pltpu.make_async_remote_copy(
                ref, ref, peer_send.at[at], peer_recv.at[at], device_id=peer, device_id_type=MESH
            ).wait_recv()

    def part_copy(buffer, at, other):
        index = buffer * TILES + at
        span = pl.ds(pl.multiple_of(at * tile, tile), tile)
        return pltpu.make_async_remote_copy(
            outgoing.at[buffer, span, :], incoming.at[buffer, span, :], part_send.at[index],
            part_recv.at[index], device_id=(band, other), device_id_type=MESH,
        )

    def product(slot, span):
        return jnp.dot(left[span, :], right[slot], preferred_element_type=jnp.float32)

    def each_tile(body):
        @pl.loop(0, TILES)
        def _(at):
            body(at, pl.ds(pl.multiple_of(at * tile, tile), tile))

    def multiply_send(slot, buffer, other):
        def body(at, span):
            outgoing[buffer, span, :] = product(slot, span).astype(jnp.bfloat16)
            part_copy(buffer, at, other).start()

        each_tile(body)

    def multiply_keep(slot, which):
        def body(at, span):
            kept[which, span, :] = product(slot, span)

        each_tile(body)

    def combine_send(which, arrived, buffer, other):
        def body(at, span):
            part_copy(arrived, at, other).wait_recv()
            total = kept[which, span, :] + incoming[arrived, span, :].astype(jnp.float32)
            outgoing[buffer, span, :] = total.astype(jnp.bfloat16)
            part_copy(buffer, at, other).start()

        each_tile(body)

    def multiply_own(slot, side):
        def body(at, span):
            columns = slice(side * half, (side + 1) * half)
            out_ref[span, columns] = result[span, columns] - product(slot, span)

        each_tile(body)

    load_left.wait()
    part_scale = scale_ref[:, pl.ds(pl.multiple_of(lane * share, share), share)]

    def scale_tile(at, span):
        left[span, :] = (left_raw[span, :].astype(jnp.float32) * part_scale).astype(jnp.bfloat16)

    each_tile(scale_tile)

    forward(0)
    await_peer(0)
    load_result.wait()
    multiply_own(0, 0)
    forward(1)
    await_peer(1)
    multiply_send(1, 2, lane_x)
    forward(2)
    await_peer(2)
    multiply_send(2, 1, lane_y)
    forward(3)
    await_peer(3)
    multiply_send(3, 3, lane_y)
    forward(4)
    await_peer(4)
    multiply_send(4, 0, lane_x)
    forward(5)
    await_peer(5)
    multiply_keep(5, 0)
    forward(6)
    await_peer(6)
    multiply_keep(6, 1)
    combine_send(0, 1, 4, lane_x)
    if EARLY:
        combine_send(1, 0, 5, lane_y)
        forward(7)
        await_peer(7)
        multiply_own(7, 1)
    else:
        forward(7)
        combine_send(1, 0, 5, lane_y)
        await_peer(7)
        multiply_own(7, 1)

    def finish(at, span):
        for buffer in (2, 3, 4, 5):
            part_copy(buffer, at, lane_x).wait_recv()
        first = out_ref[span, :half] - (
            incoming[2, span, :].astype(jnp.float32) + incoming[5, span, :].astype(jnp.float32)
        )
        second = out_ref[span, half:] - (
            incoming[3, span, :].astype(jnp.float32) + incoming[4, span, :].astype(jnp.float32)
        )
        out_ref[span, :half] = first
        out_ref[span, half:] = second
        power = first * first + second * second
        power = sum(power[:, k : k + 128] for k in range(0, half, 128))
        norm_out[:, span] = jnp.sum(power.T.reshape(16, 8, tile), axis=0)

    each_tile(finish)

    norms = [
        pltpu.make_async_remote_copy(
            norm_out, norm_in.at[k], norm_send.at[k], norm_recv.at[k],
            device_id=(band, other), device_id_type=MESH,
        )
        for k, other in enumerate((lane_x, lane_y, lane_d))
    ]
    for copy in norms:
        copy.start()

    @pl.when(lane != z)
    def _():
        for i in range(2):
            for part in range(PIECES):
                send_own(i, part).wait_send()

    for slot in range(8):
        for part in range(PIECES):
            along(slot, part, peer, peer_send, peer_recv).wait_send()

    @pl.when((z >= lane) & (z < chips - 1))
    def _():
        for slot in range(8):
            for part in range(PIECES):
                along(slot, part, above, up_sem, right_sem).wait_send()

    @pl.when((z <= lane) & (z > 0))
    def _():
        for slot in range(8):
            for part in range(PIECES):
                along(slot, part, below, down_sem, right_sem).wait_send()

    for buffer in range(6):
        for at in range(TILES):
            part_copy(buffer, at, lane_x).wait_send()

    for copy in norms:
        copy.wait()
    power = norm_out[...] + norm_in[0] + norm_in[1] + norm_in[2]
    power = jnp.sum(power, axis=0, keepdims=True)
    power_ref[...] = jnp.broadcast_to(power, (128, rows)).T


def on_device(chips, first_factor, second_factor, result_in, pivot_scale):
    rows, share = first_factor.shape
    depth, width = second_factor.shape
    half = width // 2
    slots = 8 * PIECES
    dma = pltpu.SemaphoreType.DMA
    flops = 2 * rows * share * 4 * width
    updated, power = pl.pallas_call(
        functools.partial(kernel, chips),
        out_shape=(
            jax.ShapeDtypeStruct((rows, width), jnp.float32),
            jax.ShapeDtypeStruct((rows, 128), jnp.float32),
        ),
        in_specs=[pl.BlockSpec(memory_space=pl.ANY)] * 3
        + [pl.BlockSpec(memory_space=pltpu.VMEM)],
        out_specs=[pl.BlockSpec(memory_space=pltpu.VMEM)] * 2,
        scratch_shapes=[
            pltpu.VMEM((rows, share), jnp.bfloat16),
            pltpu.VMEM((rows, share), jnp.bfloat16),
            pltpu.VMEM((8, share, half), jnp.bfloat16),
            pltpu.VMEM((rows, width), jnp.float32),
            pltpu.VMEM((6, rows, half), jnp.bfloat16),
            pltpu.VMEM((6, rows, half), jnp.bfloat16),
            pltpu.VMEM((2, rows, half), jnp.float32),
            pltpu.VMEM((8, rows), jnp.float32),
            pltpu.VMEM((3, 8, rows), jnp.float32),
            dma((2,)),
            dma((2 * PIECES,)),
            dma((slots,)),
            dma((slots,)),
            dma((slots,)),
            dma((slots,)),
            dma((slots,)),
            dma((6 * TILES,)),
            dma((6 * TILES,)),
            dma((3,)),
            dma((3,)),
        ],
        compiler_params=pltpu.CompilerParams(
            collective_id=0, has_side_effects=True, vmem_limit_bytes=VMEM
        ),
        cost_estimate=pl.CostEstimate(
            flops=flops, bytes_accessed=8 * rows * share, transcendentals=0
        ),
    )(first_factor, second_factor, result_in, pivot_scale.reshape(1, -1))
    return updated * lax.rsqrt(power[:, :1] / (width * lax.axis_size("lane")) + 1e-06)


def solution(mesh):
    bands, lanes = mesh.shape["band"], mesh.shape["lane"]

    def body(first_factor, second_factor, result_in, pivot_scale):
        fits = lanes == 4 and bands == 2 * lanes
        plan = functools.partial(on_device, bands // 2) if fits else gathered
        return plan(first_factor, second_factor, result_in, pivot_scale)

    return jax.shard_map(
        body,
        mesh=mesh,
        in_specs=(P("band", "lane"), P("band", "lane"), P("band", "lane"), P()),
        out_specs=P("band", "lane"),
        check_vma=False,
    )
```

```python
import functools

import jax
import jax.numpy as jnp
from jax import lax
from jax.experimental import pallas as pl
from jax.experimental.pallas import tpu as pltpu
from jax.sharding import PartitionSpec as P

MESH = pl.DeviceIdType.MESH
PIECES = 4
TILES = 2


def gathered(first_factor, second_factor, result_in, pivot_scale):
    share = first_factor.shape[1]
    part_scale = lax.dynamic_slice_in_dim(pivot_scale, lax.axis_index("lane") * share, share)
    scaled_left = (first_factor.astype(jnp.float32) * part_scale).astype(jnp.bfloat16)
    left_line = lax.all_gather(scaled_left, "lane", axis=1, tiled=True)
    right = lax.all_gather(second_factor, "band", axis=0, tiled=True)
    updated = result_in - jnp.dot(left_line, right, preferred_element_type=jnp.float32)
    row_power = lax.psum(jnp.sum(updated * updated, axis=1), "lane")
    return (
        updated * lax.rsqrt(row_power / (updated.shape[1] * lax.axis_size("lane")) + 1e-06)[:, None]
    )


def kernel(
    chips, left_hbm, right_hbm, result_hbm, scale_ref, out_ref, power_ref,
    left_raw, left, right, result, outgoing, incoming, kept, norm_out, norm_in,
    load_sem, source_sem, right_sem, up_sem, down_sem, peer_send, peer_recv, part_send, part_recv,
    norm_send, norm_recv,
):
    band, lane = lax.axis_index("band"), lax.axis_index("lane")
    z, core = band // 2, band % 2
    y, x = lane // 2, lane % 2
    peer = (2 * z + 1 - core, lane)
    lane_x, lane_y, lane_d = 2 * y + 1 - x, 2 * (1 - y) + x, 2 * (1 - y) + 1 - x
    above, below = (band + 2, lane), (band - 2, lane)
    depth, width = right_hbm.shape
    half = width // 2
    piece = depth // PIECES
    rows, share = left.shape
    tile = rows // TILES

    load_left = pltpu.make_async_copy(left_hbm, left_raw, load_sem.at[0])
    load_left.start()
    load_result = pltpu.make_async_copy(result_hbm, result, load_sem.at[1])
    load_result.start()

    barrier = pltpu.get_barrier_semaphore()
    for other in (lane_x, lane_y, lane_d):
        pl.semaphore_signal(barrier, inc=1, device_id=(band, other), device_id_type=MESH)
    pl.semaphore_signal(barrier, inc=1, device_id=peer, device_id_type=MESH)

    @pl.when(z < chips - 1)
    def _():
        pl.semaphore_signal(barrier, inc=1, device_id=above, device_id_type=MESH)

    @pl.when(z > 0)
    def _():
        pl.semaphore_signal(barrier, inc=1, device_id=below, device_id_type=MESH)

    pl.semaphore_wait(barrier, 4 + (z + chips - 1) // chips + (2 * chips - 2 - z) // chips)

    def place(slot, part, of_core):
        start = pl.multiple_of(of_core * depth + part * piece, piece)
        return right.at[slot, pl.ds(start, piece), :]

    dx, dy = (x + z % 2) % 2, (y + z // 2) % 2
    slot_0 = dx * (1 - dy) + 6 * (1 - dx) * dy + 4 * dx * dy
    slot_1 = 7 * (1 - dx) * (1 - dy) + 5 * dx * (1 - dy) + 3 * (1 - dx) * dy + 2 * dx * dy

    def own_block(i, part):
        side = (i + dy) % 2
        slot = slot_0 * (1 - side) + slot_1 * side
        block = right_hbm.at[
            pl.ds(part * piece, piece), pl.ds(pl.multiple_of(side * half, half), half)
        ]
        return block, slot

    def send_own(i, part):
        block, slot = own_block(i, part)
        return pltpu.make_async_remote_copy(
            block, place(slot, part, core), source_sem.at[i * PIECES + part],
            right_sem.at[slot * PIECES + part], device_id=(band, z), device_id_type=MESH,
        )

    @pl.when(lane != z)
    def _():
        for i in range(2):
            for part in range(PIECES):
                send_own(i, part).start()

    @pl.when(lane == z)
    def _():
        for i in range(2):
            for part in range(PIECES):
                block, slot = own_block(i, part)
                pltpu.make_async_copy(
                    block, place(slot, part, core), right_sem.at[slot * PIECES + part]
                ).start()

    def along(slot, part, device, send, recv):
        at = slot * PIECES + part
        ref = place(slot, part, core)
        return pltpu.make_async_remote_copy(
            ref, ref, send.at[at], recv.at[at], device_id=device, device_id_type=MESH
        )

    def forward(slot):
        for part in range(PIECES):
            along(slot, part, peer, peer_send, right_sem).wait_recv()

            @pl.when((z >= lane) & (z < chips - 1))
            def _():
                along(slot, part, above, up_sem, right_sem).start()

            @pl.when((z <= lane) & (z > 0))
            def _():
                along(slot, part, below, down_sem, right_sem).start()

            along(slot, part, peer, peer_send, peer_recv).start()

    def await_peer(slot):
        for part in range(PIECES):
            at = slot * PIECES + part
            ref = place(slot, part, 1 - core)
            pltpu.make_async_remote_copy(
                ref, ref, peer_send.at[at], peer_recv.at[at], device_id=peer, device_id_type=MESH
            ).wait_recv()

    def part_copy(buffer, at, other):
        index = buffer * TILES + at
        span = pl.ds(pl.multiple_of(at * tile, tile), tile)
        return pltpu.make_async_remote_copy(
            outgoing.at[buffer, span, :], incoming.at[buffer, span, :], part_send.at[index],
            part_recv.at[index], device_id=(band, other), device_id_type=MESH,
        )

    def product(slot, span):
        return jnp.dot(left[span, :], right[slot], preferred_element_type=jnp.float32)

    def each_tile(body):
        @pl.loop(0, TILES)
        def _(at):
            body(at, pl.ds(pl.multiple_of(at * tile, tile), tile))

    def multiply_send(slot, buffer, other):
        def body(at, span):
            outgoing[buffer, span, :] = product(slot, span).astype(jnp.bfloat16)
            part_copy(buffer, at, other).start()

        each_tile(body)

    def multiply_keep(slot, which):
        def body(at, span):
            kept[which, span, :] = product(slot, span)

        each_tile(body)

    def combine_send(which, arrived, buffer, other):
        def body(at, span):
            part_copy(arrived, at, other).wait_recv()
            total = kept[which, span, :] + incoming[arrived, span, :].astype(jnp.float32)
            outgoing[buffer, span, :] = total.astype(jnp.bfloat16)
            part_copy(buffer, at, other).start()

        each_tile(body)

    def multiply_own(slot, side):
        def body(at, span):
            columns = slice(side * half, (side + 1) * half)
            out_ref[span, columns] = result[span, columns] - product(slot, span)

        each_tile(body)

    forward(0)
    load_left.wait()
    part_scale = scale_ref[:, pl.ds(pl.multiple_of(lane * share, share), share)]

    def scale_tile(at, span):
        left[span, :] = (left_raw[span, :].astype(jnp.float32) * part_scale).astype(jnp.bfloat16)

    each_tile(scale_tile)

    await_peer(0)
    load_result.wait()
    multiply_own(0, 0)
    forward(1)
    await_peer(1)
    multiply_send(1, 2, lane_x)
    forward(2)
    await_peer(2)
    multiply_send(2, 1, lane_y)
    forward(3)
    await_peer(3)
    multiply_send(3, 3, lane_y)
    forward(4)
    await_peer(4)
    multiply_send(4, 0, lane_x)
    forward(5)
    await_peer(5)
    multiply_keep(5, 0)
    forward(6)
    await_peer(6)
    multiply_keep(6, 1)
    combine_send(0, 1, 4, lane_x)
    combine_send(1, 0, 5, lane_y)
    forward(7)
    await_peer(7)
    multiply_own(7, 1)

    def finish(at, span):
        for buffer in (2, 3, 4, 5):
            part_copy(buffer, at, lane_x).wait_recv()
        first = out_ref[span, :half] - (
            incoming[2, span, :].astype(jnp.float32) + incoming[5, span, :].astype(jnp.float32)
        )
        second = out_ref[span, half:] - (
            incoming[3, span, :].astype(jnp.float32) + incoming[4, span, :].astype(jnp.float32)
        )
        out_ref[span, :half] = first
        out_ref[span, half:] = second
        power = first * first + second * second
        power = sum(power[:, k : k + 128] for k in range(0, half, 128))
        norm_out[:, span] = jnp.sum(power.T.reshape(16, 8, tile), axis=0)

    each_tile(finish)

    norms = [
        pltpu.make_async_remote_copy(
            norm_out, norm_in.at[k], norm_send.at[k], norm_recv.at[k],
            device_id=(band, other), device_id_type=MESH,
        )
        for k, other in enumerate((lane_x, lane_y, lane_d))
    ]
    for copy in norms:
        copy.start()

    @pl.when(lane != z)
    def _():
        for i in range(2):
            for part in range(PIECES):
                send_own(i, part).wait_send()

    for slot in range(8):
        for part in range(PIECES):
            along(slot, part, peer, peer_send, peer_recv).wait_send()

    @pl.when((z >= lane) & (z < chips - 1))
    def _():
        for slot in range(8):
            for part in range(PIECES):
                along(slot, part, above, up_sem, right_sem).wait_send()

    @pl.when((z <= lane) & (z > 0))
    def _():
        for slot in range(8):
            for part in range(PIECES):
                along(slot, part, below, down_sem, right_sem).wait_send()

    for buffer in range(6):
        for at in range(TILES):
            part_copy(buffer, at, lane_x).wait_send()

    for copy in norms:
        copy.wait()
    power = norm_out[...] + norm_in[0] + norm_in[1] + norm_in[2]
    power = jnp.sum(power, axis=0, keepdims=True)
    power_ref[...] = jnp.broadcast_to(power, (128, rows)).T


def on_device(chips, first_factor, second_factor, result_in, pivot_scale):
    rows, share = first_factor.shape
    depth, width = second_factor.shape
    half = width // 2
    slots = 8 * PIECES
    dma = pltpu.SemaphoreType.DMA
    flops = 2 * rows * share * 4 * width
    updated, power = pl.pallas_call(
        functools.partial(kernel, chips),
        out_shape=(
            jax.ShapeDtypeStruct((rows, width), jnp.float32),
            jax.ShapeDtypeStruct((rows, 128), jnp.float32),
        ),
        in_specs=[
            pl.BlockSpec(memory_space=pltpu.HBM),
            pl.BlockSpec(memory_space=pl.ANY),
            pl.BlockSpec(memory_space=pl.ANY),
            pl.BlockSpec(memory_space=pltpu.VMEM),
        ],
        out_specs=[pl.BlockSpec(memory_space=pltpu.VMEM)] * 2,
        scratch_shapes=[
            pltpu.VMEM((rows, share), jnp.bfloat16),
            pltpu.VMEM((rows, share), jnp.bfloat16),
            pltpu.VMEM((8, share, half), jnp.bfloat16),
            pltpu.VMEM((rows, width), jnp.float32),
            pltpu.VMEM((6, rows, half), jnp.bfloat16),
            pltpu.VMEM((6, rows, half), jnp.bfloat16),
            pltpu.VMEM((2, rows, half), jnp.float32),
            pltpu.VMEM((8, rows), jnp.float32),
            pltpu.VMEM((3, 8, rows), jnp.float32),
            dma((2,)),
            dma((2 * PIECES,)),
            dma((slots,)),
            dma((slots,)),
            dma((slots,)),
            dma((slots,)),
            dma((slots,)),
            dma((6 * TILES,)),
            dma((6 * TILES,)),
            dma((3,)),
            dma((3,)),
        ],
        compiler_params=pltpu.CompilerParams(
            collective_id=0, has_side_effects=True, vmem_limit_bytes=48 * 1024 * 1024
        ),
        cost_estimate=pl.CostEstimate(
            flops=flops, bytes_accessed=8 * rows * share, transcendentals=0
        ),
    )(first_factor, second_factor, result_in, pivot_scale.reshape(1, -1))
    return updated * lax.rsqrt(power[:, :1] / (width * lax.axis_size("lane")) + 1e-06)


def solution(mesh):
    bands, lanes = mesh.shape["band"], mesh.shape["lane"]

    def body(first_factor, second_factor, result_in, pivot_scale):
        fits = lanes == 4 and bands == 2 * lanes
        plan = functools.partial(on_device, bands // 2) if fits else gathered
        return plan(first_factor, second_factor, result_in, pivot_scale)

    return jax.shard_map(
        body,
        mesh=mesh,
        in_specs=(P("band", "lane"), P("band", "lane"), P("band", "lane"), P()),
        out_specs=P("band", "lane"),
        check_vma=False,
    )
```
